32 devices in a mesh: gx: 8 (over y, x, core), gy: 4 (over z).
Axes of the slice: x: 2, y: 2, z: 4, core: 2. Of those that a mesh axis runs over, the one named last changes fastest.
Arguments:
- probes: bfloat16 [256, 1024, 256], P('gx', 'gy'), may hold values from -6 to 6
- blk_rows: int32 [1024, 128], P(('gx', 'gy')), may hold values from 0 to 8191
- blk_sensor: int32 [1024], P(('gx', 'gy')), may hold values from 0 to 255, as said below
- blk_count: int32 [32], P(('gx', 'gy')), may hold values from 16 to 32, as said below
- coef: bfloat16 [1024, 128], P(('gx', 'gy')), may hold values from -5 to 5
- owner: int32 [256], replicated, may hold values from 0 to 31, as said below
- weights: float32 [256], replicated, may hold values from 0.1 to 1
Outputs:
- sensitivity: float32 [256], P(('gx', 'gy'))
- new_weights: float32 [256], replicated
- density: float32 [256, 1024], P('gx', 'gy')
The draws below stay inside these ranges and needn't reach their ends.
Inputs may be any that keep to these rules, and one draw needn't show every extreme that they name: `owner`: every device owns exactly 8 sensors. `blk_sensor`: among the live slots of one tile, at most 2 belong to sensors of one owner; in every draw some owner receives 2 live blocks from every tile. `blk_count`: some tile has all 32 slots live.
All inputs are finite; a program needn't handle non-finite values.
Results may differ from the reference program's by a relative error of at most 0.0008.
Values may be sent and summed in bfloat16 or wider, within the bound.
A program may use at most 128 MiB of HBM per device.

```python
import math
import jax
import jax.numpy as jnp
from jax import lax

P_SIZE = 256
FOOT = 128
TR = 32
TC = 256
SPD = 8
CAP = 2
SENSORS = 256
NBLK = 32
GR = 256
GC = 1024
N_GX = 8
N_GY = 4
DEVICES = 32


def layout(key):
    perm = jax.random.permutation(jax.random.fold_in(key, 11), SENSORS).astype(jnp.int32)
    owners = perm // SPD
    inverse = jnp.argsort(perm, stable=True).astype(jnp.int32)
    hot = jax.random.permutation(jax.random.fold_in(key, 12), DEVICES)[:2].astype(jnp.int32)
    entries = jnp.arange(DEVICES * CAP, dtype=jnp.int32)
    is_hot = jnp.any((entries // CAP)[:, None] == hot[None, :], axis=1).astype(jnp.int32)
    score = jax.random.randint(jax.random.fold_in(key, 13), (DEVICES, DEVICES * CAP), 0, 2 ** 20, dtype=jnp.int32)
    score = (score + is_hot[None, :] * 2 ** 21) * (DEVICES * CAP) + entries[None, :]
    chosen = lax.top_k(score, NBLK)[1].astype(jnp.int32)
    dest = chosen // CAP
    within = jax.random.randint(jax.random.fold_in(key, 14), (DEVICES, NBLK), 0, SPD, dtype=jnp.int32)
    sensor = inverse[dest * SPD + within]
    count = jax.random.randint(jax.random.fold_in(key, 15), (DEVICES,), NBLK // 2, NBLK + 1, dtype=jnp.int32)
    full_tile = jax.random.randint(jax.random.fold_in(key, 16), (), 0, DEVICES, dtype=jnp.int32)
    count = jnp.where(jnp.arange(DEVICES, dtype=jnp.int32) == full_tile, NBLK, count)
    return (owners, sensor.reshape(-1), count)


def draw_owner(key, part):
    return layout(key)[0]


def draw_blk_sensor(key, part):
    return layout(key)[1]


def draw_blk_count(key, part):
    return layout(key)[2]


def touch_ends(values, own_key, least, top_value):
    longest = values.shape.index(max(values.shape))
    spots = []
    for shift in (0, 1):
        where = [jax.random.randint(jax.random.fold_in(own_key, axis), (), 0, length) for axis, length in enumerate(values.shape)]
        where[longest] = (where[longest] + shift) % values.shape[longest]
        spots.append(tuple(where))
    return values.at[spots[0]].set(least).at[spots[1]].set(top_value)


def block_levels(key, dims, shards, smallest, high):
    loudness = 1.0
    for position, blocks in shards:
        steps = jax.random.uniform(jax.random.fold_in(jax.random.fold_in(key, 6), position), (blocks,), jnp.float32, smallest / len(shards), high / len(shards))
        loudness = loudness * jnp.repeat(jnp.exp(steps), dims[position] // blocks).reshape((-1,) + (1,) * (len(dims) - 1 - position))
    return loudness


def normal_values(key, extent, deviation, limit, cuts=(), kind=jnp.bfloat16):
    values = deviation * jax.random.normal(key, extent, jnp.float32)
    if cuts:
        values = values * block_levels(key, extent, cuts, -0.22, 0.18)
    return jnp.clip(values, -limit, limit).astype(kind)


def setup_inputs(seed: int = 0) -> dict:
    keys = jax.random.split(jax.random.key(seed), 8)
    return {
        "probes": normal_values(keys[0], (GR, GC, P_SIZE), 1.0, 6.0, ((0, 8), (1, 4))),
        "blk_rows": touch_ends(jax.random.randint(keys[1], (DEVICES * NBLK, FOOT), 0, TR * TC), jax.random.fold_in(keys[1], 1), 0, (TR * TC) - 1).astype(jnp.int32),
        "blk_sensor": draw_blk_sensor(jax.random.fold_in(keys[7], 71), 0),
        "blk_count": draw_blk_count(jax.random.fold_in(keys[7], 71), 0),
        "coef": normal_values(keys[4], (DEVICES * NBLK, FOOT), 1.0, 5.0, ((0, 32),)),
        "owner": draw_owner(jax.random.fold_in(keys[7], 71), 0),
        "weights": jnp.clip(jnp.exp(jax.random.uniform(keys[6], (SENSORS,), jnp.float32, math.log(0.1), math.log(1.0))), 0.1, 1.0),
    }


def reference(probes, blk_rows, blk_sensor, blk_count, coef, owner, weights):
    tiles = probes.reshape(N_GX, TR, N_GY, TC, P_SIZE).transpose(0, 2, 1, 3, 4).reshape(N_GX * N_GY, TR * TC, P_SIZE)
    rows = blk_rows.reshape(DEVICES, NBLK, FOOT)
    sensors = blk_sensor.reshape(DEVICES, NBLK)
    coefs = coef.reshape(DEVICES, NBLK, FOOT)
    live = (jnp.arange(NBLK, dtype=jnp.int32)[None, :] < blk_count[:, None]).astype(jnp.float32)

    def accumulate(obs, inputs):
        tile, row_ids, sens, weight, alive = inputs
        picked = tile[row_ids.reshape(-1)].reshape(NBLK, FOOT, P_SIZE).astype(jnp.float32)
        contrib = weight.astype(jnp.float32)[:, :, None] * picked * alive[:, None, None]
        return (obs.at[sens].add(contrib), None)
    obs = lax.scan(accumulate, jnp.zeros((SENSORS, FOOT, P_SIZE), jnp.float32), (tiles, rows, sensors, coefs, live))[0]
    sens_h = lax.optimization_barrier(jnp.sum(obs * obs, axis=(1, 2))) / (FOOT * P_SIZE)
    order = jnp.argsort(owner * SENSORS + jnp.arange(SENSORS, dtype=jnp.int32))
    sensitivity = sens_h[order]
    gain = weights * jnp.sqrt(1.0 + sens_h)
    new_weights = SENSORS * gain / jnp.sum(gain)
    values = live[:, :, None] * new_weights[sensors][:, :, None] * jnp.square(coefs.astype(jnp.float32))
    tile_ids = jnp.broadcast_to(jnp.arange(DEVICES, dtype=jnp.int32)[:, None, None], rows.shape)
    dens = jnp.zeros((DEVICES, TR * TC), jnp.float32).at[tile_ids, rows].add(values)
    density = dens.reshape(N_GX, N_GY, TR, TC).transpose(0, 2, 1, 3).reshape(N_GX * TR, N_GY * TC)
    return (sensitivity, new_weights, density)
```

```python
import functools

import jax
import jax.numpy as jnp
from jax import lax
from jax.experimental import pallas as pl
from jax.experimental.pallas import tpu as pltpu
from jax.sharding import PartitionSpec as P

MESH = pl.DeviceIdType.MESH
F32 = jnp.float32
BF16 = jnp.bfloat16
NT = (((1,), (1,)), ((), ()))
LANES = 128


def gather_kernel(n, rows_ref, coef_ref, probes_ref, out_ref, tile_ref, stage_ref):
    tile_r, tile_c, probe_n = probes_ref.shape
    chans, nblk = stage_ref.shape[:2]

    def widen(i, carry):
        at = pl.multiple_of(i * tile_c, tile_c)
        tile_ref[pl.ds(at, tile_c), :] = probes_ref[i].astype(F32)
        return carry

    lax.fori_loop(0, tile_r, widen, 0)

    def fill(d, carry):
        for c in range(chans):
            r = d * chans + c
            for j in range(nblk):
                i = rows_ref[j, r]
                stage_ref[c, pl.ds(j, 1), :] = tile_ref[pl.ds(i, 1), :] * coef_ref[j, r]
            out_ref[d, :, c * probe_n : (c + 1) * probe_n] = stage_ref[c].astype(BF16)
        return carry

    lax.fori_loop(0, n, fill, 0)


def exchange_kernel(
    n, n_gy, scale, tile_c,
    send_ref, ids_ref, ids_col_ref, rows_ref, coef_ref, owner_ref, weights_ref,
    owned_ref, new_ref, density_ref,
    recv_ref, ids_recv, obs_ref, planes_ref, h_send, h_recv,
    send_sem, recv_sem, ids_send_sem, ids_recv_sem, h_send_sem, h_recv_sem,
):
    me = lax.axis_index("gx") * n_gy + lax.axis_index("gy")
    nblk, width = send_ref.shape[1:]
    n_sens = owner_ref.shape[1]
    tile_r = density_ref.shape[0]
    share = max(1, LANES // nblk)

    def peer(k):
        t = lax.rem(me + k, n)
        return t, (t // n_gy, lax.rem(t, n_gy))

    barrier = pltpu.get_barrier_semaphore()

    def greet(k, carry):
        pl.semaphore_signal(barrier, inc=1, device_id=peer(k)[1], device_id_type=MESH)
        return carry

    lax.fori_loop(1, n, greet, 0)
    own = pltpu.make_async_copy(send_ref.at[me], recv_ref.at[me], recv_sem.at[me])
    own_ids = pltpu.make_async_copy(ids_ref, ids_recv.at[me], ids_recv_sem.at[me])
    own.start()
    own_ids.start()
    pl.semaphore_wait(barrier, n - 1)

    def block_copy(k):
        t, where = peer(k)
        return pltpu.make_async_remote_copy(
            src_ref=send_ref.at[t], dst_ref=recv_ref.at[me],
            send_sem=send_sem.at[k], recv_sem=recv_sem.at[me],
            device_id=where, device_id_type=MESH,
        )

    def ids_copy(k):
        return pltpu.make_async_remote_copy(
            src_ref=ids_ref, dst_ref=ids_recv.at[me],
            send_sem=ids_send_sem.at[k], recv_sem=ids_recv_sem.at[me],
            device_id=peer(k)[1], device_id_type=MESH,
        )

    def h_copy(k):
        return pltpu.make_async_remote_copy(
            src_ref=h_send, dst_ref=h_recv.at[me],
            send_sem=h_send_sem.at[k], recv_sem=h_recv_sem.at[me],
            device_id=peer(k)[1], device_id_type=MESH,
        )

    def launch(k, carry):
        ids_copy(k).start()
        block_copy(k).start()
        return carry

    lax.fori_loop(1, n, launch, 0)

    def plane(j, carry):
        at = rows_ref[pl.ds(j, 1), :]
        c = coef_ref[pl.ds(j, 1), :]
        square = c * c
        top = square.astype(BF16).astype(F32)
        high = at // tile_c
        low = at - high * tile_c
        here = high == lax.broadcasted_iota(jnp.int32, (tile_r, at.shape[1]), 0)
        left = jnp.concatenate(
            [jnp.where(here, top, 0.0), jnp.where(here, square - top, 0.0)], axis=0
        ).astype(BF16)
        right = jnp.where(
            low == lax.broadcasted_iota(jnp.int32, (tile_c, at.shape[1]), 0), 1.0, 0.0
        ).astype(BF16)
        both = lax.dot_general(left, right, NT, preferred_element_type=F32)
        planes_ref[j] = both[:tile_r] + both[tile_r:]
        return carry

    lax.fori_loop(0, nblk, plane, 0)

    spd = n_sens // n
    mine = jnp.where(owner_ref[...] == me, 1.0, 0.0)
    before = jnp.where(
        lax.broadcasted_iota(jnp.int32, (n_sens, n_sens), 0)
        < lax.broadcasted_iota(jnp.int32, (n_sens, n_sens), 1),
        1.0, 0.0,
    ).astype(BF16)
    rank = jnp.dot(
        jnp.broadcast_to(mine, (spd, n_sens)).astype(BF16), before, preferred_element_type=F32
    )
    place = lax.broadcasted_iota(jnp.int32, (spd, n_sens), 0).astype(F32)
    select = jnp.where(rank == place, 1.0, 0.0) * mine

    def ids_wait(t, carry):
        pltpu.make_async_copy(ids_ref, ids_recv.at[t], ids_recv_sem.at[t]).wait()
        return carry

    lax.fori_loop(0, n, ids_wait, 0)

    group = max(1, 256 // nblk)
    depth = group * nblk
    obs_ref[...] = jnp.zeros_like(obs_ref)

    def mix(g, carry):
        pieces = []
        for piece in range(depth // LANES):
            row = ids_recv[g * group + piece * share]
            for extra in range(1, share):
                row = row + ids_recv[g * group + piece * share + extra]
            pieces.append(row)
        ids_row = jnp.concatenate(pieces, axis=1)
        mixer = jnp.where(
            ids_row == lax.broadcasted_iota(jnp.int32, (n_sens, depth), 0) + 1, 1.0, 0.0
        ).astype(BF16)
        for piece in range(group):
            t = g * group + piece
            pltpu.make_async_copy(send_ref.at[0], recv_ref.at[t], recv_sem.at[t]).wait()
        block = recv_ref[pl.ds(g * group, group)].reshape(depth, width)
        obs_ref[...] += jnp.dot(mixer, block, preferred_element_type=F32)
        return carry

    lax.fori_loop(0, n // group, mix, 0)

    eye = lax.broadcasted_iota(jnp.int32, (LANES, LANES), 0) == lax.broadcasted_iota(
        jnp.int32, (LANES, LANES), 1
    )
    for b in range(n_sens // LANES):
        x = obs_ref[b * LANES : (b + 1) * LANES, :]
        s = jnp.sum(x * x, axis=1, keepdims=True)
        h_send[:, b * LANES : (b + 1) * LANES] = jnp.sum(
            jnp.where(eye, s, 0.0), axis=0, keepdims=True
        )
    h_recv[me] = h_send[...]

    def h_launch(k, carry):
        h_copy(k).start()
        return carry

    lax.fori_loop(1, n, h_launch, 0)

    def h_wait(k, carry):
        t = peer(k)[0]
        pltpu.make_async_copy(h_send, h_recv.at[t], h_recv_sem.at[t]).wait()
        return carry

    lax.fori_loop(1, n, h_wait, 0)
    h = jnp.sum(h_recv[...], axis=0) * scale
    gain = weights_ref[...] * jnp.sqrt(1.0 + h)
    new = n_sens * gain / jnp.sum(gain, axis=1, keepdims=True)
    new_ref[...] = new
    owned_ref[...] = jnp.sum(select * h, axis=1, keepdims=True)
    lookup = (
        ids_col_ref[...] == lax.broadcasted_iota(jnp.int32, (nblk, n_sens), 1) + 1
    )
    factor = jnp.sum(jnp.where(lookup, new, 0.0), axis=1, keepdims=True)
    total = factor[0:1] * planes_ref[0]
    for j in range(1, nblk):
        total = total + factor[j : j + 1] * planes_ref[j]
    density_ref[...] = total

    def drain(k, carry):
        block_copy(k).wait_send()
        ids_copy(k).wait_send()
        h_copy(k).wait_send()
        return carry

    lax.fori_loop(1, n, drain, 0)


def local(n, n_gy, probes, blk_rows, blk_sensor, blk_count, coef, owner, weights):
    tile_r, tile_c, probe_n = probes.shape
    nblk, foot = blk_rows.shape
    n_sens = owner.shape[0]
    chans = foot // n
    width = chans * probe_n
    me = lax.axis_index("gx") * n_gy + lax.axis_index("gy")
    coef32 = coef.astype(F32)
    slots = jnp.arange(nblk, dtype=jnp.int32)
    ids = jnp.where(slots < blk_count[0], blk_sensor + 1, 0)
    share = max(1, LANES // nblk)
    part = jnp.arange(share, dtype=jnp.int32)[:, None] == me % share
    ids_row = jnp.where(part, ids[None, :], 0).reshape(1, share * nblk)

    vmem = pl.BlockSpec(memory_space=pltpu.VMEM)
    smem = pl.BlockSpec(memory_space=pltpu.SMEM)
    send = pl.pallas_call(
        functools.partial(gather_kernel, n),
        out_shape=jax.ShapeDtypeStruct((n, nblk, width), BF16),
        in_specs=[smem, smem, vmem],
        out_specs=vmem,
        scratch_shapes=[
            pltpu.VMEM((tile_r * tile_c, probe_n), F32),
            pltpu.VMEM((chans, nblk, probe_n), F32),
        ],
        compiler_params=pltpu.CompilerParams(vmem_limit_bytes=40 * 2**20),
        name="gather_rows",
    )(blk_rows, coef32, probes)

    dma = pltpu.SemaphoreType.DMA
    owned, new, density = pl.pallas_call(
        functools.partial(exchange_kernel, n, n_gy, 1.0 / (foot * probe_n), tile_c),
        out_shape=(
            jax.ShapeDtypeStruct((n_sens // n, 1), F32),
            jax.ShapeDtypeStruct((1, n_sens), F32),
            jax.ShapeDtypeStruct((tile_r, tile_c), F32),
        ),
        in_specs=[vmem] * 7,
        out_specs=(vmem, vmem, vmem),
        scratch_shapes=[
            pltpu.VMEM((n, nblk, width), BF16),
            pltpu.VMEM((n, 1, share * nblk), jnp.int32),
            pltpu.VMEM((n_sens, width), F32),
            pltpu.VMEM((nblk, tile_r, tile_c), F32),
            pltpu.VMEM((1, n_sens), F32),
            pltpu.VMEM((n, 1, n_sens), F32),
            dma((n,)), dma((n,)), dma((n,)), dma((n,)), dma((n,)), dma((n,)),
        ],
        compiler_params=pltpu.CompilerParams(
            collective_id=0, has_side_effects=True, vmem_limit_bytes=48 * 2**20
        ),
        name="exchange_mix",
    )(
        send, ids_row, ids.reshape(nblk, 1), blk_rows, coef32,
        owner.reshape(1, n_sens), weights.reshape(1, n_sens),
    )
    return owned.reshape(-1), new.reshape(-1), density


def solution(mesh):
    n_gy = mesh.shape["gy"]
    n = mesh.shape["gx"] * n_gy
    in_specs = (
        P("gx", "gy", None),
        P(("gx", "gy"), None),
        P(("gx", "gy")),
        P(("gx", "gy")),
        P(("gx", "gy"), None),
        P(),
        P(),
    )
    out_specs = (P(("gx", "gy")), P(), P("gx", "gy"))
    return jax.shard_map(
        functools.partial(local, n, n_gy),
        mesh=mesh, in_specs=in_specs, out_specs=out_specs, check_vma=False,
    )
```

```python
import functools

import jax
import jax.numpy as jnp
from jax import lax
from jax.experimental import pallas as pl
from jax.experimental.pallas import tpu as pltpu
from jax.sharding import PartitionSpec as P

MESH = pl.DeviceIdType.MESH
F32 = jnp.float32
BF16 = jnp.bfloat16
NT = (((1,), (1,)), ((), ()))
LANES = 128


def step_kernel(
    n, n_gy, scale,
    rows_sm, count_sm, probes_hbm, sensor_ref, rows_ref, coef_ref, owner_ref, weights_ref,
    owned_ref, new_ref, density_ref,
    probes_ref, tile_ref, stage_ref, coef32_ref, send_ref, recv_ref, ids_send, ids_recv,
    obs_ref, planes_ref, h_send, h_recv,
    load_sem, send_sem, recv_sem, ids_send_sem, ids_recv_sem, h_send_sem, h_recv_sem,
):
    me = lax.axis_index("gx") * n_gy + lax.axis_index("gy")
    nblk, width = send_ref.shape[1:]
    tile_r, tile_c, probe_n = probes_ref.shape
    chans = stage_ref.shape[0]
    n_sens = owner_ref.shape[1]
    foot = coef_ref.shape[1]
    wide = ids_send.shape[1]
    share = wide // nblk

    def peer(k):
        t = lax.rem(me + k, n)
        return t, (t // n_gy, lax.rem(t, n_gy))

    barrier = pltpu.get_barrier_semaphore()

    def greet(k, carry):
        pl.semaphore_signal(barrier, inc=1, device_id=peer(k)[1], device_id_type=MESH)
        return carry

    parts = load_sem.shape[0]
    span = tile_r // parts

    def load(q):
        at = pl.ds(q * span, span)
        return pltpu.make_async_copy(probes_hbm.at[at], probes_ref.at[at], load_sem.at[q])

    for q in range(parts):
        load(q).start()
    lax.fori_loop(1, n, greet, 0)

    coef32_ref[...] = coef_ref[...].astype(F32)
    slot = lax.broadcasted_iota(jnp.int32, (1, nblk), 1)
    ids_one = jnp.where(slot < count_sm[0], sensor_ref[...] + 1, 0).astype(F32)
    down = lax.broadcasted_iota(jnp.int32, (nblk, nblk), 0)
    ids_col = jnp.sum(
        jnp.where(down == lax.broadcasted_iota(jnp.int32, (nblk, nblk), 1), ids_one, 0.0),
        axis=1, keepdims=True,
    )
    offset = lax.rem(me, share) * nblk
    ids_send[...] = jnp.sum(
        jnp.where(
            lax.broadcasted_iota(jnp.int32, (nblk, wide), 1)
            == lax.broadcasted_iota(jnp.int32, (nblk, wide), 0) + offset,
            ids_col, 0.0,
        ),
        axis=0, keepdims=True,
    )
    ids_recv[me] = ids_send[...]

    for q in range(parts):
        load(q).wait()

        def widen(i, carry):
            at = pl.multiple_of(i * tile_c, tile_c)
            tile_ref[pl.ds(at, tile_c), :] = probes_ref[i].astype(F32)
            return carry

        lax.fori_loop(q * span, (q + 1) * span, widen, 0)

    pl.semaphore_wait(barrier, n - 1)

    def block_copy(k):
        t, where = peer(k)
        return pltpu.make_async_remote_copy(
            src_ref=send_ref.at[t], dst_ref=recv_ref.at[me],
            send_sem=send_sem.at[k], recv_sem=recv_sem.at[me],
            device_id=where, device_id_type=MESH,
        )

    def ids_copy(k):
        return pltpu.make_async_remote_copy(
            src_ref=ids_send, dst_ref=ids_recv.at[me],
            send_sem=ids_send_sem.at[k], recv_sem=ids_recv_sem.at[me],
            device_id=peer(k)[1], device_id_type=MESH,
        )

    def h_copy(k):
        return pltpu.make_async_remote_copy(
            src_ref=h_send, dst_ref=h_recv.at[me],
            send_sem=h_send_sem.at[k], recv_sem=h_recv_sem.at[me],
            device_id=peer(k)[1], device_id_type=MESH,
        )

    channel = lax.broadcasted_iota(jnp.int32, (nblk, foot), 1)

    def gather(d):
        for c in range(chans):
            r = d * chans + c
            for j in range(nblk):
                i = rows_sm[j, r]
                stage_ref[c, pl.ds(j, 1), :] = tile_ref[pl.ds(i, 1), :]
            column = jnp.sum(
                jnp.where(channel == r, coef32_ref[...], 0.0), axis=1, keepdims=True
            )
            send_ref[d, :, c * probe_n : (c + 1) * probe_n] = (stage_ref[c] * column).astype(BF16)

    def launch(k, carry):
        gather(peer(k)[0])

        @pl.when(k > 1)
        def _():
            block_copy(k - 1).start()
            ids_copy(k - 1).start()

        return carry

    lax.fori_loop(1, n + 1, launch, 0)
    own = pltpu.make_async_copy(send_ref.at[me], recv_ref.at[me], recv_sem.at[me])

    def plane(j, carry):
        at = rows_ref[pl.ds(j, 1), :]
        c = coef32_ref[pl.ds(j, 1), :]
        square = c * c
        top = square.astype(BF16).astype(F32)
        high = at // tile_c
        low = at - high * tile_c
        here = high == lax.broadcasted_iota(jnp.int32, (tile_r, foot), 0)
        left = jnp.concatenate(
            [jnp.where(here, top, 0.0), jnp.where(here, square - top, 0.0)], axis=0
        ).astype(BF16)
        right = jnp.where(
            low == lax.broadcasted_iota(jnp.int32, (tile_c, foot), 0), 1.0, 0.0
        ).astype(BF16)
        both = lax.dot_general(left, right, NT, preferred_element_type=F32)
        planes_ref[j] = both[:tile_r] + both[tile_r:]
        return carry

    lax.fori_loop(0, nblk, plane, 0)
    own.start()

    spd = n_sens // n
    mine = jnp.where(owner_ref[...] == me, 1.0, 0.0)
    before = jnp.where(
        lax.broadcasted_iota(jnp.int32, (n_sens, n_sens), 0)
        < lax.broadcasted_iota(jnp.int32, (n_sens, n_sens), 1),
        1.0, 0.0,
    ).astype(BF16)
    rank = jnp.dot(
        jnp.broadcast_to(mine, (spd, n_sens)).astype(BF16), before, preferred_element_type=F32
    )
    place = lax.broadcasted_iota(jnp.int32, (spd, n_sens), 0).astype(F32)
    select = jnp.where(rank == place, 1.0, 0.0) * mine

    def ids_wait(k, carry):
        t = peer(k)[0]
        pltpu.make_async_copy(ids_send, ids_recv.at[t], ids_recv_sem.at[t]).wait()
        return carry

    lax.fori_loop(1, n, ids_wait, 0)

    group = max(1, 256 // nblk)
    depth = group * nblk
    obs_ref[...] = jnp.zeros_like(obs_ref)
    sensor_up = (lax.broadcasted_iota(jnp.int32, (n_sens, depth), 0) + 1).astype(F32)

    def mix(g, carry):
        pieces = []
        for piece in range(depth // wide):
            row = ids_recv[g * group + piece * share]
            for extra in range(1, share):
                row = row + ids_recv[g * group + piece * share + extra]
            pieces.append(row)
        ids_row = jnp.concatenate(pieces, axis=1)
        mixer = jnp.where(ids_row == sensor_up, 1.0, 0.0).astype(BF16)
        for piece in range(group):
            t = g * group + piece
            pltpu.make_async_copy(send_ref.at[0], recv_ref.at[t], recv_sem.at[t]).wait()
        block = recv_ref[pl.ds(g * group, group)].reshape(depth, width)
        obs_ref[...] += jnp.dot(mixer, block, preferred_element_type=F32)
        return carry

    lax.fori_loop(0, n // group, mix, 0)

    eye = lax.broadcasted_iota(jnp.int32, (LANES, LANES), 0) == lax.broadcasted_iota(
        jnp.int32, (LANES, LANES), 1
    )
    for b in range(n_sens // LANES):
        x = obs_ref[b * LANES : (b + 1) * LANES, :]
        s = jnp.sum(x * x, axis=1, keepdims=True)
        h_send[:, b * LANES : (b + 1) * LANES] = jnp.sum(
            jnp.where(eye, s, 0.0), axis=0, keepdims=True
        )
    h_recv[me] = h_send[...]

    def h_launch(k, carry):
        h_copy(k).start()
        return carry

    lax.fori_loop(1, n, h_launch, 0)

    def drain(k, carry):
        block_copy(k).wait_send()
        ids_copy(k).wait_send()
        return carry

    lax.fori_loop(1, n, drain, 0)

    def h_wait(k, carry):
        t = peer(k)[0]
        pltpu.make_async_copy(h_send, h_recv.at[t], h_recv_sem.at[t]).wait()
        return carry

    lax.fori_loop(1, n, h_wait, 0)
    h = jnp.sum(h_recv[...], axis=0) * scale
    gain = weights_ref[...] * jnp.sqrt(1.0 + h)
    new = n_sens * gain / jnp.sum(gain, axis=1, keepdims=True)
    new_ref[...] = new
    owned = jnp.sum(select * h, axis=1, keepdims=True)
    small = lax.broadcasted_iota(jnp.int32, (spd, spd), 0) == lax.broadcasted_iota(
        jnp.int32, (spd, spd), 1
    )
    owned_ref[...] = jnp.sum(jnp.where(small, owned, 0.0), axis=0, keepdims=True)
    lookup = ids_col == (lax.broadcasted_iota(jnp.int32, (nblk, n_sens), 1) + 1).astype(F32)
    factor = jnp.sum(jnp.where(lookup, new, 0.0), axis=1, keepdims=True)
    total = factor[0:1] * planes_ref[0]
    for j in range(1, nblk):
        total = total + factor[j : j + 1] * planes_ref[j]
    density_ref[...] = total

    def h_drain(k, carry):
        h_copy(k).wait_send()
        return carry

    lax.fori_loop(1, n, h_drain, 0)


def local(n, n_gy, probes, blk_rows, blk_sensor, blk_count, coef, owner, weights):
    tile_r, tile_c, probe_n = probes.shape
    nblk, foot = blk_rows.shape
    n_sens = owner.shape[0]
    chans = foot // n
    width = chans * probe_n
    wide = max(LANES, nblk)

    vmem = pl.BlockSpec(memory_space=pltpu.VMEM)
    smem = pl.BlockSpec(memory_space=pltpu.SMEM)
    dma = pltpu.SemaphoreType.DMA
    owned, new, density = pl.pallas_call(
        functools.partial(step_kernel, n, n_gy, 1.0 / (foot * probe_n)),
        out_shape=(
            jax.ShapeDtypeStruct((1, n_sens // n), F32),
            jax.ShapeDtypeStruct((1, n_sens), F32),
            jax.ShapeDtypeStruct((tile_r, tile_c), F32),
        ),
        in_specs=[smem, smem, pl.BlockSpec(memory_space=pl.ANY)] + [vmem] * 5,
        out_specs=(vmem, vmem, vmem),
        scratch_shapes=[
            pltpu.VMEM((tile_r, tile_c, probe_n), BF16),
            pltpu.VMEM((tile_r * tile_c, probe_n), F32),
            pltpu.VMEM((chans, nblk, probe_n), F32),
            pltpu.VMEM((nblk, foot), F32),
            pltpu.VMEM((n, nblk, width), BF16),
            pltpu.VMEM((n, nblk, width), BF16),
            pltpu.VMEM((1, wide), F32),
            pltpu.VMEM((n, 1, wide), F32),
            pltpu.VMEM((n_sens, width), F32),
            pltpu.VMEM((nblk, tile_r, tile_c), F32),
            pltpu.VMEM((1, n_sens), F32),
            pltpu.VMEM((n, 1, n_sens), F32),
            dma((4,)), dma((n,)), dma((n,)), dma((n,)), dma((n,)), dma((n,)), dma((n,)),
        ],
        compiler_params=pltpu.CompilerParams(
            collective_id=0, has_side_effects=True, vmem_limit_bytes=61 * 2**20
        ),
        name="reweight_step",
    )(
        blk_rows, blk_count, probes, blk_sensor.reshape(1, nblk), blk_rows, coef,
        owner.reshape(1, n_sens), weights.reshape(1, n_sens),
    )
    return owned.reshape(-1), new.reshape(-1), density


def solution(mesh):
    n_gy = mesh.shape["gy"]
    n = mesh.shape["gx"] * n_gy
    in_specs = (
        P("gx", "gy", None),
        P(("gx", "gy"), None),
        P(("gx", "gy")),
        P(("gx", "gy")),
        P(("gx", "gy"), None),
        P(),
        P(),
    )
    out_specs = (P(("gx", "gy")), P(), P("gx", "gy"))
    return jax.shard_map(
        functools.partial(local, n, n_gy),
        mesh=mesh, in_specs=in_specs, out_specs=out_specs, check_vma=False,
    )
```

```python
import functools

import jax
import jax.numpy as jnp
from jax import lax
from jax.experimental import pallas as pl
from jax.experimental.pallas import tpu as pltpu
from jax.sharding import PartitionSpec as P

MESH = pl.DeviceIdType.MESH
F32 = jnp.float32
BF16 = jnp.bfloat16
NT = (((1,), (1,)), ((), ()))
LANES = 128


def step_kernel(
    n, n_gy, scale,
    rows_sm, count_sm, probes_hbm, sensor_ref, rows_ref, coef_ref, owner_ref, weights_ref,
    owned_ref, new_ref, density_ref,
    probes_ref, tile_ref, stage_ref, coef32_ref, send_ref, recv_ref, ids_send, ids_recv,
    obs_ref, planes_ref, h_send, h_recv,
    load_sem, send_sem, recv_sem, ids_send_sem, ids_recv_sem, h_send_sem, h_recv_sem,
    *merge_refs,
):
    m, hz = n // 2, n_gy // 2
    half = lax.axis_index("gy") // hz
    inner = lax.axis_index("gx") * hz + lax.rem(lax.axis_index("gy"), hz)
    me = half * m + inner
    flat = lax.axis_index("gx") * n_gy + lax.axis_index("gy")
    nblk, width = send_ref.shape[1:]
    tile_r, tile_c, probe_n = probes_ref.shape
    chans = width // probe_n
    merge = bool(merge_refs)
    if merge:
        (send_m, recv_m, obs_m, part_send, part_recv,
         send_m_sem, recv_m_sem, part_send_sem, part_recv_sem) = merge_refs
        chans_m = send_m.shape[2] // probe_n
        side = part_send.shape[1]
    else:
        chans_m = 0
    n_sens = owner_ref.shape[1]
    foot = coef_ref.shape[1]
    wide = ids_send.shape[1]
    share = wide // nblk

    def device_of(t):
        q = lax.rem(t, m)
        return (q // hz, (t // m) * hz + lax.rem(q, hz))

    def peer(k):
        t = lax.rem(me + k, n)
        return t, device_of(t)

    barrier = pltpu.get_barrier_semaphore()

    def greet(k, carry):
        pl.semaphore_signal(barrier, inc=1, device_id=peer(k)[1], device_id_type=MESH)
        return carry

    parts = load_sem.shape[0]
    span = tile_r // parts

    def load(q):
        at = pl.ds(q * span, span)
        return pltpu.make_async_copy(probes_hbm.at[at], probes_ref.at[at], load_sem.at[q])

    for q in range(parts):
        load(q).start()
    lax.fori_loop(1, n, greet, 0)

    coef32_ref[...] = coef_ref[...].astype(F32)
    slot = lax.broadcasted_iota(jnp.int32, (1, nblk), 1)
    ids_one = jnp.where(slot < count_sm[0], sensor_ref[...] + 1, 0).astype(F32)
    down = lax.broadcasted_iota(jnp.int32, (nblk, nblk), 0)
    ids_col = jnp.sum(
        jnp.where(down == lax.broadcasted_iota(jnp.int32, (nblk, nblk), 1), ids_one, 0.0),
        axis=1, keepdims=True,
    )
    offset = lax.rem(me, share) * nblk
    ids_send[...] = jnp.sum(
        jnp.where(
            lax.broadcasted_iota(jnp.int32, (nblk, wide), 1)
            == lax.broadcasted_iota(jnp.int32, (nblk, wide), 0) + offset,
            ids_col, 0.0,
        ),
        axis=0, keepdims=True,
    )
    ids_recv[me] = ids_send[...]

    for q in range(parts):
        load(q).wait()

        def widen(i, carry):
            at = pl.multiple_of(i * tile_c, tile_c)
            tile_ref[pl.ds(at, tile_c), :] = probes_ref[i].astype(F32)
            return carry

        lax.fori_loop(q * span, (q + 1) * span, widen, 0)

    pl.semaphore_wait(barrier, n - 1)

    def block_copy(t):
        return pltpu.make_async_remote_copy(
            src_ref=send_ref.at[t], dst_ref=recv_ref.at[me],
            send_sem=send_sem.at[t], recv_sem=recv_sem.at[me],
            device_id=device_of(t), device_id_type=MESH,
        )

    def merge_copy(q):
        return pltpu.make_async_remote_copy(
            src_ref=send_m.at[q], dst_ref=recv_m.at[inner],
            send_sem=send_m_sem.at[q], recv_sem=recv_m_sem.at[inner],
            device_id=device_of(half * m + q), device_id_type=MESH,
        )

    def part_copy():
        return pltpu.make_async_remote_copy(
            src_ref=part_send, dst_ref=part_recv,
            send_sem=part_send_sem, recv_sem=part_recv_sem,
            device_id=device_of((1 - half) * m + inner), device_id_type=MESH,
        )

    def ids_copy(k):
        return pltpu.make_async_remote_copy(
            src_ref=ids_send, dst_ref=ids_recv.at[me],
            send_sem=ids_send_sem.at[k], recv_sem=ids_recv_sem.at[me],
            device_id=peer(k)[1], device_id_type=MESH,
        )

    def h_copy(k):
        return pltpu.make_async_remote_copy(
            src_ref=h_send, dst_ref=h_recv.at[me],
            send_sem=h_send_sem.at[k], recv_sem=h_recv_sem.at[me],
            device_id=peer(k)[1], device_id_type=MESH,
        )

    channel = lax.broadcasted_iota(jnp.int32, (nblk, foot), 1)

    def gather(dst, d, first, count, base):
        for c in range(count):
            r = first + c
            for j in range(nblk):
                i = rows_sm[j, r]
                stage_ref[base + c, pl.ds(j, 1), :] = tile_ref[pl.ds(i, 1), :]
            column = jnp.sum(
                jnp.where(channel == r, coef32_ref[...], 0.0), axis=1, keepdims=True
            )
            dst[d, :, c * probe_n : (c + 1) * probe_n] = (stage_ref[base + c] * column).astype(BF16)

    def inside(k):
        return lax.rem(inner + k, m)

    def ids_launch(k, carry):
        ids_copy(k).start()
        return carry

    lax.fori_loop(1, n, ids_launch, 0)

    def launch_first(k, carry):
        q = inside(k)
        t = (1 - half) * m + q
        if merge:
            gather(send_m, q, q * chans_m, chans_m, 0)
        gather(send_ref, t, m * chans_m + t * chans, chans, chans_m)

        @pl.when(k > 1)
        def _():
            if merge:
                merge_copy(inside(k - 1)).start()
            block_copy((1 - half) * m + inside(k - 1)).start()

        return carry

    lax.fori_loop(1, m + 1, launch_first, 0)

    def launch_second(k, carry):
        t = half * m + inside(k)
        gather(send_ref, t, m * chans_m + t * chans, chans, 0)

        @pl.when(k == 1)
        def _():
            block_copy((1 - half) * m + inner).start()

        @pl.when(k > 1)
        def _():
            block_copy(half * m + inside(k - 1)).start()

        return carry

    lax.fori_loop(1, m + 1, launch_second, 0)
    own = pltpu.make_async_copy(send_ref.at[me], recv_ref.at[me], recv_sem.at[me])
    if merge:
        own_m = pltpu.make_async_copy(send_m.at[inner], recv_m.at[inner], recv_m_sem.at[inner])
        own_m.start()

    def plane(j, carry):
        at = rows_ref[pl.ds(j, 1), :]
        c = coef32_ref[pl.ds(j, 1), :]
        square = c * c
        top = square.astype(BF16).astype(F32)
        high = at // tile_c
        low = at - high * tile_c
        here = high == lax.broadcasted_iota(jnp.int32, (tile_r, foot), 0)
        left = jnp.concatenate(
            [jnp.where(here, top, 0.0), jnp.where(here, square - top, 0.0)], axis=0
        ).astype(BF16)
        right = jnp.where(
            low == lax.broadcasted_iota(jnp.int32, (tile_c, foot), 0), 1.0, 0.0
        ).astype(BF16)
        both = lax.dot_general(left, right, NT, preferred_element_type=F32)
        planes_ref[j] = both[:tile_r] + both[tile_r:]
        return carry

    lax.fori_loop(0, nblk, plane, 0)
    own.start()

    spd = n_sens // n
    mine = jnp.where(owner_ref[...] == flat, 1.0, 0.0)
    before = jnp.where(
        lax.broadcasted_iota(jnp.int32, (n_sens, n_sens), 0)
        < lax.broadcasted_iota(jnp.int32, (n_sens, n_sens), 1),
        1.0, 0.0,
    ).astype(BF16)
    rank = jnp.dot(
        jnp.broadcast_to(mine, (spd, n_sens)).astype(BF16), before, preferred_element_type=F32
    )
    place = lax.broadcasted_iota(jnp.int32, (spd, n_sens), 0).astype(F32)
    select = jnp.where(rank == place, 1.0, 0.0) * mine

    def ids_wait(k, carry):
        t = peer(k)[0]
        pltpu.make_async_copy(ids_send, ids_recv.at[t], ids_recv_sem.at[t]).wait()
        return carry

    lax.fori_loop(1, n, ids_wait, 0)

    group = max(1, 256 // nblk)
    depth = group * nblk
    sensor_up = (lax.broadcasted_iota(jnp.int32, (n_sens, depth), 0) + 1).astype(F32)

    def mix(src, sem, like, obs, start, g):
        pieces = []
        for piece in range(depth // wide):
            row = ids_recv[start + g * group + piece * share]
            for extra in range(1, share):
                row = row + ids_recv[start + g * group + piece * share + extra]
            pieces.append(row)
        ids_row = jnp.concatenate(pieces, axis=1)
        mixer = jnp.where(ids_row == sensor_up, 1.0, 0.0).astype(BF16)
        for piece in range(group):
            t = g * group + piece
            pltpu.make_async_copy(like, src.at[t], sem.at[t]).wait()
        block = src[pl.ds(g * group, group)].reshape(depth, src.shape[2])
        obs[...] += jnp.dot(mixer, block, preferred_element_type=F32)

    obs_ref[...] = jnp.zeros_like(obs_ref)
    if merge:
        obs_m[...] = jnp.zeros_like(obs_m)

        def mix_m(g, carry):
            mix(recv_m, recv_m_sem, send_m.at[0], obs_m, half * m, g)
            return carry

        lax.fori_loop(0, m // group, mix_m, 0)
        away = pl.multiple_of((1 - half) * side, LANES)
        part_send[...] = obs_m[:, pl.ds(away, side)].astype(BF16)
        part_copy().start()

    def mix_d(g, carry):
        mix(recv_ref, recv_sem, send_ref.at[0], obs_ref, 0, g)
        return carry

    lax.fori_loop(0, n // group, mix_d, 0)
    if merge:
        part_copy().wait()
        keep = pl.multiple_of(half * side, LANES)

    eye = lax.broadcasted_iota(jnp.int32, (LANES, LANES), 0) == lax.broadcasted_iota(
        jnp.int32, (LANES, LANES), 1
    )
    for b in range(n_sens // LANES):
        x = obs_ref[b * LANES : (b + 1) * LANES, :]
        s = jnp.sum(x * x, axis=1, keepdims=True)
        if merge:
            rows = pl.ds(b * LANES, LANES)
            y = obs_m[rows, pl.ds(keep, side)] + part_recv[rows, :].astype(F32)
            s = s + jnp.sum(y * y, axis=1, keepdims=True)
        h_send[:, b * LANES : (b + 1) * LANES] = jnp.sum(
            jnp.where(eye, s, 0.0), axis=0, keepdims=True
        )
    h_recv[me] = h_send[...]

    def h_launch(k, carry):
        h_copy(k).start()
        return carry

    lax.fori_loop(1, n, h_launch, 0)

    def drain(k, carry):
        block_copy(peer(k)[0]).wait_send()
        ids_copy(k).wait_send()
        return carry

    lax.fori_loop(1, n, drain, 0)
    if merge:

        def drain_m(k, carry):
            merge_copy(inside(k)).wait_send()
            return carry

        lax.fori_loop(1, m, drain_m, 0)

    def h_wait(k, carry):
        t = peer(k)[0]
        pltpu.make_async_copy(h_send, h_recv.at[t], h_recv_sem.at[t]).wait()
        return carry

    lax.fori_loop(1, n, h_wait, 0)
    h = jnp.sum(h_recv[...], axis=0) * scale
    gain = weights_ref[...] * jnp.sqrt(1.0 + h)
    new = n_sens * gain / jnp.sum(gain, axis=1, keepdims=True)
    new_ref[...] = new
    owned = jnp.sum(select * h, axis=1, keepdims=True)
    small = lax.broadcasted_iota(jnp.int32, (spd, spd), 0) == lax.broadcasted_iota(
        jnp.int32, (spd, spd), 1
    )
    owned_ref[...] = jnp.sum(jnp.where(small, owned, 0.0), axis=0, keepdims=True)
    lookup = ids_col == (lax.broadcasted_iota(jnp.int32, (nblk, n_sens), 1) + 1).astype(F32)
    factor = jnp.sum(jnp.where(lookup, new, 0.0), axis=1, keepdims=True)
    total = factor[0:1] * planes_ref[0]
    for j in range(1, nblk):
        total = total + factor[j : j + 1] * planes_ref[j]
    density_ref[...] = total

    def h_drain(k, carry):
        h_copy(k).wait_send()
        return carry

    lax.fori_loop(1, n, h_drain, 0)


def local(n, n_gy, probes, blk_rows, blk_sensor, blk_count, coef, owner, weights):
    tile_r, tile_c, probe_n = probes.shape
    nblk, foot = blk_rows.shape
    n_sens = owner.shape[0]
    merge = foot % (2 * n) == 0
    chans = foot // (2 * n) if merge else foot // n
    chans_m = 2 * chans if merge else 0
    width = chans * probe_n
    wide = max(LANES, nblk)

    vmem = pl.BlockSpec(memory_space=pltpu.VMEM)
    smem = pl.BlockSpec(memory_space=pltpu.SMEM)
    dma = pltpu.SemaphoreType.DMA
    merge_scratch = []
    if merge:
        m = n // 2
        merge_scratch = [
            pltpu.VMEM((m, nblk, chans_m * probe_n), BF16),
            pltpu.VMEM((m, nblk, chans_m * probe_n), BF16),
            pltpu.VMEM((n_sens, chans_m * probe_n), F32),
            pltpu.VMEM((n_sens, width), BF16),
            pltpu.VMEM((n_sens, width), BF16),
            dma((m,)), dma((m,)), dma, dma,
        ]
    owned, new, density = pl.pallas_call(
        functools.partial(step_kernel, n, n_gy, 1.0 / (foot * probe_n)),
        out_shape=(
            jax.ShapeDtypeStruct((1, n_sens // n), F32),
            jax.ShapeDtypeStruct((1, n_sens), F32),
            jax.ShapeDtypeStruct((tile_r, tile_c), F32),
        ),
        in_specs=[smem, smem, pl.BlockSpec(memory_space=pltpu.HBM)] + [vmem] * 5,
        out_specs=(vmem, vmem, vmem),
        scratch_shapes=[
            pltpu.VMEM((tile_r, tile_c, probe_n), BF16),
            pltpu.VMEM((tile_r * tile_c, probe_n), F32),
            pltpu.VMEM((chans + chans_m, nblk, probe_n), F32),
            pltpu.VMEM((nblk, foot), F32),
            pltpu.VMEM((n, nblk, width), BF16),
            pltpu.VMEM((n, nblk, width), BF16),
            pltpu.VMEM((1, wide), F32),
            pltpu.VMEM((n, 1, wide), F32),
            pltpu.VMEM((n_sens, width), F32),
            pltpu.VMEM((nblk, tile_r, tile_c), F32),
            pltpu.VMEM((1, n_sens), F32),
            pltpu.VMEM((n, 1, n_sens), F32),
            dma((4,)), dma((n,)), dma((n,)), dma((n,)), dma((n,)), dma((n,)), dma((n,)),
        ] + merge_scratch,
        compiler_params=pltpu.CompilerParams(
            collective_id=0, has_side_effects=True, vmem_limit_bytes=56 * 2**20
        ),
        name="reweight_step",
    )(
        blk_rows, blk_count, probes, blk_sensor.reshape(1, nblk), blk_rows, coef,
        owner.reshape(1, n_sens), weights.reshape(1, n_sens),
    )
    return owned.reshape(-1), new.reshape(-1), density


def solution(mesh):
    n_gy = mesh.shape["gy"]
    n = mesh.shape["gx"] * n_gy
    in_specs = (
        P("gx", "gy", None),
        P(("gx", "gy"), None),
        P(("gx", "gy")),
        P(("gx", "gy")),
        P(("gx", "gy"), None),
        P(),
        P(),
    )
    out_specs = (P(("gx", "gy")), P(), P("gx", "gy"))
    return jax.shard_map(
        functools.partial(local, n, n_gy),
        mesh=mesh, in_specs=in_specs, out_specs=out_specs, check_vma=False,
    )
```
